512 devices in a mesh: pipe: 8 (over y, core), seq: 64 (over x, z).
Axes of the slice: x: 4, y: 4, z: 16, core: 2. Of those that a mesh axis runs over, the one named last changes fastest.
Arguments:
- inputs: bfloat16 [2, 32768, 512], P(None, 'seq'), may hold values from -6 to 6
- w_in: bfloat16 [8, 512, 2048], P('pipe'), may hold values from -0.25 to 0.25
- w_out: bfloat16 [8, 512, 512], P('pipe'), may hold values from -0.25 to 0.25
- lengths: int32 [2, 16], replicated, may hold values from 1 to 8192, 32768 in all within a row
- valid: int32 [2, 64], replicated, may hold values from 128 to 512
Outputs:
- states: bfloat16 [8, 2, 32768, 512], P('pipe', None, 'seq')
The draws below stay inside these ranges and needn't reach their ends.
Inputs may be any that keep to these rules, and one draw needn't show every extreme that they name: Each row of stream lengths sums to 32768.
All inputs are finite; a program needn't handle non-finite values.
Results may differ from the reference program's by a relative error of at most 0.025.
Values may be sent and summed in bfloat16 or wider, within the bound.
A program may use at most 64 MiB of HBM per device.

```python
import math
import jax
import jax.numpy as jnp
import numpy as np
from jax import lax

D = 512
HEADS = 4
HEAD_DIM = 128
WINDOW = 512
MICRO = 2
TOK_DEV = 512
HD = 512
LAYERS = 8
ROWS = 32768
GROUPS = 64
STREAMS = 16


def place_ends(array, stream_key, low, top_value):
    longest = array.shape.index(max(array.shape))
    spots = []
    for shift in (0, 1):
        where = [jax.random.randint(jax.random.fold_in(stream_key, axis), (), 0, length) for axis, length in enumerate(array.shape)]
        where[longest] = (where[longest] + shift) % array.shape[longest]
        spots.append(tuple(where))
    return array.at[spots[0]].set(low).at[spots[1]].set(top_value)


def steps_of(own_key, shape, pieces, smallest, top_value):
    factor_of = 1.0
    for axis_at, shards_of in pieces:
        steps = jax.random.uniform(jax.random.fold_in(jax.random.fold_in(own_key, 6), axis_at), (shards_of,), jnp.float32, smallest / len(pieces), top_value / len(pieces))
        factor_of = factor_of * jnp.repeat(jnp.exp(steps), shape[axis_at] // shards_of).reshape((-1,) + (1,) * (len(shape) - 1 - axis_at))
    return factor_of


def profile(number_of, total, limit, slope):
    portions = [(1 << 20) // math.isqrt(grade ** slope) + 1 for grade in range(2, number_of + 1)]
    surplus, holding = total - limit - (number_of - 1), [1] * (number_of - 1)
    while surplus > 0:
        candidates = [i for i in range(number_of - 1) if holding[i] < limit]
        pool, left = sum([portions[i] for i in candidates]), surplus
        for i in candidates:
            extra = min(limit - holding[i], max(1, left * portions[i] // pool), surplus)
            holding[i] = holding[i] + extra
            surplus = surplus - extra
    return np.array([limit] + holding)


def uneven(key, count, total, reach, skew):
    if count == 2:
        one = jax.random.randint(key, (), max(1, total - reach), min(reach, total - 1) + 1)
        return jnp.stack([one, total - one])
    tallies = jnp.asarray(profile(count, total, reach, skew), jnp.int32)
    pairs = (count - 1) // 2
    donor, sink = tallies[1:1 + 2 * pairs:2], tallies[2:2 + 2 * pairs:2]
    slack = jnp.minimum(donor - 1, reach - sink)
    moved = jax.random.randint(jax.random.fold_in(key, 1), (pairs,), 0, 1 << 20) % (slack + 1)
    tallies = tallies.at[1:1 + 2 * pairs:2].set(donor - moved).at[2:2 + 2 * pairs:2].set(sink + moved)
    return tallies[jax.random.permutation(jax.random.fold_in(key, 2), count)]


def scatter_about(key, shape, scale, bound, cuts=(), held_as=jnp.bfloat16):
    entries = jax.random.normal(key, shape, jnp.float32) * scale
    if len(cuts) > 0:
        entries = steps_of(key, shape, cuts, -0.22, 0.18) * entries
    return jnp.clip(entries, min=-bound, max=bound).astype(held_as)


def setup_inputs(seed: int = 0) -> dict:
    splits = jax.random.split(jax.random.key(seed), 6)
    return {
        "inputs": scatter_about(splits[0], (MICRO, ROWS, D), 1.0, 6.0, ((1, 64),)),
        "w_in": scatter_about(splits[1], (LAYERS, D, 4 * HD), D ** -0.5, 0.25, ((0, 8),)),
        "w_out": scatter_about(splits[2], (LAYERS, HD, D), HD ** -0.5, 0.25, ((0, 8),)),
        "lengths": jax.vmap(lambda own: uneven(own, STREAMS, ROWS, ROWS // 4, 2))(jax.random.split(splits[3], MICRO)).reshape((MICRO, STREAMS)).astype(jnp.int32),
        "valid": place_ends(jax.random.randint(splits[4], (MICRO, GROUPS), TOK_DEV // 4, TOK_DEV + 1), jax.random.fold_in(splits[4], 1), TOK_DEV // 4, TOK_DEV).astype(jnp.int32),
    }


norm_eps = 1e-05
out_eps = 0.001

def layer_norm(values, epsilon):
    mean = lax.optimization_barrier(jnp.mean(values, axis=-1, keepdims=True))
    centred = values - mean
    spread = lax.optimization_barrier(jnp.mean(centred * centred, axis=-1, keepdims=True))
    return centred / jnp.sqrt(spread + epsilon)

def one_layer(hidden, weight_in, weight_out, bounds, valid_row):
    rows = hidden.shape[0]
    width = HEADS * HEAD_DIM
    normed = layer_norm(hidden.astype(jnp.float32), norm_eps).astype(jnp.bfloat16)
    proj = jax.nn.silu(jnp.dot(normed, weight_in, preferred_element_type=jnp.float32)).astype(jnp.bfloat16)
    gate_part = proj[:, :width]
    value_part = proj[:, width:2 * width]
    query_part = proj[:, 2 * width:3 * width]
    key_part = proj[:, 3 * width:]
    places = jnp.arange(rows, dtype=jnp.int32)
    stream = lax.optimization_barrier(jnp.sum((places[:, None] >= bounds[None, :]).astype(jnp.int32), axis=1))
    live = places % TOK_DEV < valid_row[places // TOK_DEV]
    key_pad = jnp.concatenate([jnp.zeros((WINDOW, width), key_part.dtype), key_part], 0)
    value_pad = jnp.concatenate([jnp.zeros((WINDOW, width), value_part.dtype), value_part], 0)
    stream_pad = jnp.concatenate([jnp.zeros((WINDOW,), jnp.int32) - 1, stream], 0)
    live_pad = jnp.concatenate([jnp.zeros((WINDOW,), bool), live], 0)
    span = TOK_DEV + WINDOW
    score_scale = 1.0 / math.sqrt(HEAD_DIM)
    mix_scale = 1.0 / math.sqrt(WINDOW)

    def block(index):
        start = (index * TOK_DEV).astype(jnp.int32)
        query = lax.dynamic_slice_in_dim(query_part, start, TOK_DEV, 0).astype(jnp.float32)
        keys = lax.dynamic_slice_in_dim(key_pad, start, span, 0).astype(jnp.float32)
        values = lax.dynamic_slice_in_dim(value_pad, start, span, 0).astype(jnp.float32)
        query_stream = lax.dynamic_slice_in_dim(stream, start, TOK_DEV, 0)
        key_stream = lax.dynamic_slice_in_dim(stream_pad, start, span, 0)
        query_live = lax.dynamic_slice_in_dim(live, start, TOK_DEV, 0)
        key_live = lax.dynamic_slice_in_dim(live_pad, start, span, 0)
        query_pos = start + jnp.arange(TOK_DEV, dtype=jnp.int32)
        key_pos = start - WINDOW + jnp.arange(span, dtype=jnp.int32)
        allowed = query_live[:, None] & key_live[None, :] & (query_stream[:, None] == key_stream[None, :]) & (key_pos[None, :] <= query_pos[:, None]) & (query_pos[:, None] - key_pos[None, :] < WINDOW) & (key_pos[None, :] >= 0)
        scores = jnp.einsum('qhd,khd->hqk', query.reshape(TOK_DEV, HEADS, HEAD_DIM), keys.reshape(span, HEADS, HEAD_DIM))
        weights = jnp.where(allowed[None], jax.nn.silu(scores * score_scale) * mix_scale, 0.0).astype(jnp.bfloat16)
        mixed = jnp.einsum('hqk,khd->qhd', weights.astype(jnp.float32), values.reshape(span, HEADS, HEAD_DIM))
        return mixed.reshape(TOK_DEV, width)
    attended = lax.map(block, jnp.arange(rows // TOK_DEV, dtype=jnp.int32)).reshape(rows, width)
    gated = (layer_norm(attended, out_eps) * gate_part.astype(jnp.float32)).astype(jnp.bfloat16)
    return (hidden.astype(jnp.float32) + jnp.dot(gated, weight_out, preferred_element_type=jnp.float32)).astype(jnp.bfloat16)

def reference(inputs, w_in, w_out, lengths, valid):
    results = []
    current = [inputs[m] for m in range(MICRO)]
    for layer in range(LAYERS):
        outputs = []
        for m in range(MICRO):
            bounds = jnp.cumsum(lengths[m]).astype(jnp.int32)
            outputs.append(one_layer(current[m], w_in[layer], w_out[layer], bounds, valid[m]))
        results.append(jnp.stack(outputs, 0))
        current = outputs
    return jnp.stack(results, 0)
```

```python
import functools
import math

import jax
import jax.numpy as jnp
from jax import lax
from jax.experimental import pallas as pl
from jax.experimental.pallas import tpu as pltpu
from jax.sharding import PartitionSpec as P

MESH = pl.DeviceIdType.MESH

HEAD_DIM = 128
WINDOW = 512
CH = 128
BF = jnp.bfloat16
F32 = jnp.float32

norm_eps = 1e-05
out_eps = 0.001


def half_silu(h):
    h = h.astype(BF)
    return h + h * jnp.tanh(h)


def kernel(micro, tok, width, hd, sections, blocks, streams,
           inp, win, wout, lens, valid, out,
           xin, hn, nb, w1, w2, qb, ub, kb, vb, mask,
           ld_sem, xs, xr, hs, hr):
    p = lax.axis_index("pipe")
    b = lax.axis_index("seq")
    heads = hd // HEAD_DIM
    span = WINDOW + CH
    n_ch = tok // CH
    right = lax.rem(b + 1, blocks)
    left = lax.rem(b + blocks - 1, blocks)
    up = lax.rem(p + 1, sections)
    down = lax.rem(p + sections - 1, sections)

    barrier = pltpu.get_barrier_semaphore()
    for dev in ((p, left), (p, right), (up, b), (down, b)):
        pl.semaphore_signal(barrier, inc=1, device_id=dev, device_id_type=MESH)

    load_in = pltpu.make_async_copy(win.at[0], w1, ld_sem.at[0])
    load_out = pltpu.make_async_copy(wout.at[0], w2, ld_sem.at[1])
    load_x = pltpu.make_async_copy(inp, xin, ld_sem.at[2])

    @pl.when(p == 0)
    def _():
        load_x.start()

    load_in.start()
    load_out.start()

    score_scale = 0.5 / math.sqrt(HEAD_DIM)
    ii = lax.broadcasted_iota(jnp.int32, (CH, 1), 0)
    jj = lax.broadcasted_iota(jnp.int32, (1, span), 1)

    def make_mask(step, carry):
        m = step // n_ch
        k = lax.rem(step, n_ch)
        row = k * CH + ii
        col = k * CH + jj - WINDOW
        q_pos = b * tok + row
        k_pos = b * tok + col
        q_stream = jnp.zeros_like(q_pos)
        k_stream = jnp.zeros_like(k_pos)
        bound = jnp.int32(0)
        for n in range(streams):
            bound = bound + lens[m, n]
            q_stream = q_stream + jnp.where(q_pos >= bound, 1, 0)
            k_stream = k_stream + jnp.where(k_pos >= bound, 1, 0)
        here = valid[m, b]
        before = valid[m, left]
        k_count = jnp.where(col >= 0, here, before)
        k_row = jnp.where(col >= 0, col, col + tok)
        k_code = jnp.where((k_row < k_count) & (k_pos >= 0), k_stream, -1)
        q_code = jnp.where(row < here, q_stream, -2)
        ok = (q_code == k_code) & (jj > ii) & (jj <= ii + WINDOW)
        mask[m, k] = jnp.where(ok, score_scale, 0.0)
        return carry

    lax.fori_loop(0, micro * n_ch, make_mask, 0)

    pl.semaphore_wait(barrier, 4)

    @pl.when(p == 0)
    def _():
        load_x.wait()

    load_in.wait()
    load_out.wait()

    def x_copy(m, k):
        rows = pl.ds(pl.multiple_of(k * CH, CH), CH)
        return pltpu.make_async_remote_copy(
            src_ref=out.at[0, m, rows], dst_ref=xin.at[m, rows],
            send_sem=xs.at[m, k], recv_sem=xr.at[m, k],
            device_id=(up, b), device_id_type=MESH)

    def h_copy(m, k):
        rows = pl.ds(pl.multiple_of(k * CH, CH), CH)
        return pltpu.make_async_remote_copy(
            src_ref=nb.at[m, rows], dst_ref=hn.at[m, rows],
            send_sem=hs.at[m, k], recv_sem=hr.at[m, k],
            device_id=(p, right), device_id_type=MESH)

    def own(m, step):
        k = n_ch - 1 - step
        base = pl.multiple_of(k * CH, CH)
        rows = pl.ds(base, CH)

        @pl.when(p > 0)
        def _():
            x_copy(m, k).wait_recv()

        x = xin[m, rows].astype(F32)
        mean = jnp.mean(x, axis=-1, keepdims=True)
        cen = x - mean
        var = jnp.mean(cen * cen, axis=-1, keepdims=True)
        nrm = (cen * (0.5 * lax.rsqrt(var + norm_eps))).astype(BF)
        nb[m, rows] = nrm
        h_copy(m, k).start()
        own_rows = pl.ds(pl.multiple_of(WINDOW + base, CH), CH)
        for ref, at, rr in ((ub, 0, rows), (vb, 1, own_rows), (qb, 2, rows), (kb, 3, own_rows)):
            ref[rr] = half_silu(jnp.dot(
                nrm, w1[:, at * hd:(at + 1) * hd], preferred_element_type=F32))

    def attend(m, step):
        k = n_ch - 1 - step
        base = pl.multiple_of(k * CH, CH)
        rows = pl.ds(base, CH)
        h_copy(m, k).wait_recv()
        nrm = hn[m, rows]
        for ref, at in ((kb, 3), (vb, 1)):
            ref[rows] = half_silu(jnp.dot(
                nrm, w1[:, at * hd:(at + 1) * hd], preferred_element_type=F32))
        keys = pl.ds(base, span)
        mk = mask[m, k]
        parts = []
        for h in range(heads):
            cols = slice(h * HEAD_DIM, (h + 1) * HEAD_DIM)
            s = lax.dot_general(qb[rows, cols], kb[keys, cols], (((1,), (1,)), ((), ())),
                                preferred_element_type=F32)
            a = half_silu(s * mk)
            parts.append(jnp.dot(a, vb[keys, cols], preferred_element_type=F32))
        att = jnp.concatenate(parts, 1)
        mean = jnp.mean(att, axis=-1, keepdims=True)
        cen = att - mean
        var = jnp.mean(cen * cen, axis=-1, keepdims=True)
        gated = (cen * lax.rsqrt(var + out_eps * WINDOW) * ub[rows].astype(F32)).astype(BF)
        res = xin[m, rows].astype(F32) + jnp.dot(gated, w2[...], preferred_element_type=F32)
        out[0, m, rows] = res.astype(BF)

        @pl.when(p < sections - 1)
        def _():
            x_copy(m, k).start()

    for m in range(micro):
        def own_step(step, carry, m=m):
            own(m, step)
            return carry

        def att_step(step, carry, m=m):
            attend(m, step)
            return carry

        lax.fori_loop(0, n_ch, own_step, 0)
        lax.fori_loop(0, n_ch, att_step, 0)

    for m in range(micro):
        for k in range(n_ch):
            h_copy(m, k).wait_send()

            @pl.when(p < sections - 1)
            def _():
                x_copy(m, k).wait_send()


def shards(mesh, inputs, w_in, w_out, lengths, valid):
    micro, tok, width = inputs.shape
    hd = w_out.shape[1]
    sections = mesh.shape["pipe"]
    blocks = mesh.shape["seq"]
    streams = lengths.shape[1]
    n_ch = tok // CH
    hbm = pl.BlockSpec(memory_space=pl.ANY)
    smem = pl.BlockSpec(memory_space=pltpu.SMEM)
    return pl.pallas_call(
        functools.partial(kernel, micro, tok, width, hd, sections, blocks, streams),
        out_shape=jax.ShapeDtypeStruct((1, micro, tok, width), BF),
        in_specs=[hbm, hbm, hbm, smem, smem],
        out_specs=pl.BlockSpec(memory_space=pltpu.VMEM),
        scratch_shapes=[
            pltpu.VMEM((micro, tok, width), BF),
            pltpu.VMEM((micro, tok, width), BF),
            pltpu.VMEM((micro, tok, width), BF),
            pltpu.VMEM((width, 4 * hd), BF),
            pltpu.VMEM((hd, width), BF),
            pltpu.VMEM((tok, hd), BF),
            pltpu.VMEM((tok, hd), BF),
            pltpu.VMEM((WINDOW + tok, hd), BF),
            pltpu.VMEM((WINDOW + tok, hd), BF),
            pltpu.VMEM((micro, n_ch, CH, WINDOW + CH), F32),
            pltpu.SemaphoreType.DMA((3,)),
            pltpu.SemaphoreType.DMA((micro, n_ch)),
            pltpu.SemaphoreType.DMA((micro, n_ch)),
            pltpu.SemaphoreType.DMA((micro, n_ch)),
            pltpu.SemaphoreType.DMA((micro, n_ch)),
        ],
        compiler_params=pltpu.CompilerParams(
            collective_id=0, has_side_effects=True, vmem_limit_bytes=48 << 20),
    )(inputs, w_in, w_out, lengths, valid)


def solution(mesh):
    in_specs = (P(None, "seq", None), P("pipe", None, None), P("pipe", None, None), P(), P())
    out_specs = P("pipe", None, "seq", None)
    return jax.shard_map(functools.partial(shards, mesh), mesh=mesh, in_specs=in_specs,
                         out_specs=out_specs, check_vma=False)
```

```python
import functools
import math

import jax
import jax.numpy as jnp
from jax import lax
from jax.experimental import pallas as pl
from jax.experimental.pallas import tpu as pltpu
from jax.sharding import PartitionSpec as P

MESH = pl.DeviceIdType.MESH

HEAD_DIM = 128
WINDOW = 512
CH = 128
SUB = 64
HELPERS = (2, 6)
BF = jnp.bfloat16
F32 = jnp.float32

norm_eps = 1e-05
out_eps = 0.001


def half_silu(h):
    h = h.astype(BF)
    return h + h * jnp.tanh(h)


def centred(x, epsilon):
    mean = jnp.mean(x, axis=-1, keepdims=True)
    cen = x - mean
    return cen, lax.rsqrt(jnp.mean(cen * cen, axis=-1, keepdims=True) + epsilon)


def kernel(micro, tok, width, hd, sections, blocks, streams,
           inp, win, wout, lens_hbm, valid_hbm, out,
           ob, xin, hx, w1, w2, qb, ub, kb, vb, acc, mask, lens, valid,
           ld_sem, out_sem, xs, xr, hs, hr, fs, js):
    p = lax.axis_index("pipe")
    b = lax.axis_index("seq")
    heads = hd // HEAD_DIM
    span = WINDOW + CH
    n_ch = tok // CH
    n_sub = CH // SUB
    right = lax.rem(b + 1, blocks)
    left = lax.rem(b + blocks - 1, blocks)
    up = lax.rem(p + 1, sections)
    down = lax.rem(p + sections - 1, sections)
    even = lax.rem(p, 2) == 0
    last = p == sections - 1

    barrier = pltpu.get_barrier_semaphore()
    for dev in ((p, left), (p, right), (up, b), (down, b), (up, right), (down, left)):
        pl.semaphore_signal(barrier, inc=1, device_id=dev, device_id_type=MESH)

    @pl.when(p == 0)
    def _():
        for helper in HELPERS:
            pl.semaphore_signal(barrier, inc=1, device_id=(helper, left), device_id_type=MESH)

    load_x = pltpu.make_async_copy(inp, xin, ld_sem.at[0])
    load_in = pltpu.make_async_copy(win.at[0], w1, ld_sem.at[1])
    load_out = pltpu.make_async_copy(wout.at[0], w2, ld_sem.at[2])
    load_len = pltpu.make_async_copy(lens_hbm, lens, ld_sem.at[3])
    load_val = pltpu.make_async_copy(valid_hbm, valid, ld_sem.at[4])

    @pl.when(p == 0)
    def _():
        load_x.start()

    load_len.start()
    load_val.start()
    load_in.start()
    load_out.start()

    def sub_rows(k, j):
        return pl.ds(pl.multiple_of(k * CH + j * SUB, SUB), SUB)

    def x_copy(m, k, j):
        return pltpu.make_async_remote_copy(
            src_ref=ob.at[m, sub_rows(k, j)], dst_ref=xin.at[m, sub_rows(k, j)],
            send_sem=xs.at[m, k, j], recv_sem=xr.at[m, k, j],
            device_id=(up, b), device_id_type=MESH)

    def h_copy(m, k, j):
        return pltpu.make_async_remote_copy(
            src_ref=xin.at[m, sub_rows(k, j)], dst_ref=hx.at[m, sub_rows(k, j)],
            send_sem=hs.at[m, k, j], recv_sem=hr.at[m, k, j],
            device_id=(p, right), device_id_type=MESH)

    def i_copy(m, k, j):
        return pltpu.make_async_remote_copy(
            src_ref=inp.at[m, sub_rows(k, j)], dst_ref=hx.at[m, sub_rows(k, j)],
            send_sem=js.at[m, k, j], recv_sem=hr.at[m, k, j],
            device_id=(0, right), device_id_type=MESH)

    def f_copy(m, k, j):
        return pltpu.make_async_remote_copy(
            src_ref=ob.at[m, sub_rows(k, j)], dst_ref=hx.at[m, sub_rows(k, j)],
            send_sem=fs.at[m, k, j], recv_sem=hr.at[m, k, j],
            device_id=(up, right), device_id_type=MESH)

    def rows_of(k):
        return pl.ds(pl.multiple_of(k * CH, CH), CH)

    def out_copy(m, k):
        return pltpu.make_async_copy(
            ob.at[m, rows_of(k)], out.at[0, m, rows_of(k)], out_sem.at[m, k])

    first_sends = {0: [(0, 3), (0, 0)], HELPERS[0]: [(0, 2), (1, 3), (1, 1)],
                   HELPERS[1]: [(0, 1), (1, 2), (1, 0)]}
    helps = (p == HELPERS[0]) | (p == HELPERS[1])
    pl.semaphore_wait(barrier, jnp.where(helps, 7, 6))

    for sender, pieces in first_sends.items():
        @pl.when(p == sender)
        def _():
            for m, k in pieces:
                for j in range(n_sub):
                    i_copy(m, k, j).start()

    @pl.when(p == 0)
    def _():
        load_x.wait()

    load_len.wait()
    load_val.wait()

    score_scale = 0.5 / math.sqrt(HEAD_DIM)
    ii = lax.broadcasted_iota(jnp.int32, (CH, 1), 0)
    jj = lax.broadcasted_iota(jnp.int32, (1, span), 1)

    def make_mask(step, carry):
        m = step // n_ch
        k = lax.rem(step, n_ch)
        row = k * CH + ii
        col = k * CH + jj - WINDOW
        q_pos = b * tok + row
        k_pos = b * tok + col
        q_stream = jnp.zeros_like(q_pos)
        k_stream = jnp.zeros_like(k_pos)
        bound = jnp.int32(0)
        for n in range(streams):
            bound = bound + lens[m, n]
            q_stream = q_stream + jnp.where(q_pos >= bound, 1, 0)
            k_stream = k_stream + jnp.where(k_pos >= bound, 1, 0)
        here = valid[m, b]
        before = valid[m, left]
        k_count = jnp.where(col >= 0, here, before)
        k_row = jnp.where(col >= 0, col, col + tok)
        k_code = jnp.where((k_row < k_count) & (k_pos >= 0), k_stream, -1)
        q_code = jnp.where(row < here, q_stream, -2)
        ok = (q_code == k_code) & (jj > ii) & (jj <= ii + WINDOW)
        mask[m, k] = jnp.where(ok, score_scale, 0.0)
        return carry

    lax.fori_loop(0, micro * n_ch, make_mask, 0)
    load_in.wait()
    load_out.wait()

    def project(x, targets):
        cen, rstd = centred(x.astype(F32), norm_eps)
        cen = cen.astype(BF)
        for ref, at, rows in targets:
            ref[rows] = half_silu(jnp.dot(
                cen, w1[:, at * hd:(at + 1) * hd], preferred_element_type=F32) * (0.5 * rstd))

    def weigh(m, q, lo, hi):
        rows = slice(q * CH, (q + 1) * CH)
        keys = slice(lo * CH, hi * CH)
        mk = mask[m, q, :, (lo - q) * CH:(hi - q) * CH]
        raw = [lax.dot_general(qb[rows, c], kb[keys, c], (((1,), (1,)), ((), ())),
                               preferred_element_type=F32) for c in head_cols]
        return lo, hi, [half_silu(s * mk) for s in raw]

    def mix(weighed):
        lo, hi, weights = weighed
        keys = slice(lo * CH, hi * CH)
        return jnp.concatenate([jnp.dot(w, vb[keys, c], preferred_element_type=F32)
                                for w, c in zip(weights, head_cols)], 1)

    head_cols = [slice(h * HEAD_DIM, (h + 1) * HEAD_DIM) for h in range(heads)]
    lead = WINDOW // CH

    def chunk(k):
        return slice(k * CH, (k + 1) * CH)

    def gather_weights(m, j):
        return [(q, weigh(m, q, lead + j, lead + j + 1)) for q in range(j, n_ch)]

    def gather_mix(j, weighed):
        for q, w in weighed:
            acc[chunk(q)] = mix(w) if q == j else acc[chunk(q)] + mix(w)

    def own(m, k):
        @pl.when(p > 0)
        def _():
            for j in range(n_sub):
                x_copy(m, k, j).wait_recv()
                if k > 0:
                    @pl.when(even)
                    def _():
                        h_copy(m, k, j).start()

        weighed = gather_weights(m, k + 1) if 0 < k < n_ch - 1 else None
        at = chunk(lead + k)
        project(xin[m, chunk(k)],
                ((kb, 3, at), (vb, 1, at), (qb, 2, chunk(k)), (ub, 0, chunk(k))))
        if weighed:
            gather_mix(k + 1, weighed)

    def attend(m, k):
        rows = chunk(k)
        for j in range(n_sub):
            h_copy(m, k, j).wait_recv()
        ahead = weigh(m, k - 1, k + 1, lead + 1) if k > 0 else None
        close = weigh(m, k, lead, lead + 1) if k == n_ch - 1 else None
        project(hx[m, rows], ((kb, 3, rows), (vb, 1, rows)))
        att = acc[rows]
        if close:
            att = att + mix(close)
        if ahead:
            got = mix(ahead)
        tail = weigh(m, k, k, k + 1)
        if ahead:
            more = weigh(m, k - 1, k, k + 1)
        att = att + mix(tail)
        if ahead:
            got = got + mix(more)
            acc[chunk(k - 1)] = got if k == 1 else acc[chunk(k - 1)] + got
        cen, rstd = centred(att, out_eps * WINDOW)
        gated = (cen * ub[rows].astype(F32)).astype(BF)
        res = xin[m, rows].astype(F32) + rstd * jnp.dot(
            gated, w2[...], preferred_element_type=F32)
        ob[m, rows] = res.astype(BF)
        out_copy(m, k).start()

        @pl.when(jnp.logical_not(last))
        def _():
            for j in range(n_sub):
                x_copy(m, k, j).start()

        @pl.when(jnp.logical_not(last) if k == 0 else even)
        def _():
            for j in range(n_sub):
                f_copy(m, k, j).start()

    def layer(m, carry):
        for k in range(n_ch - 1, -1, -1):
            if k == 0:
                gather_mix(1, gather_weights(m, 1))
            own(m, k)
        for k in range(n_ch - 1, -1, -1):
            attend(m, k)
        return carry

    lax.fori_loop(0, micro, layer, 0)

    for sender, pieces in first_sends.items():
        @pl.when(p == sender)
        def _():
            for m, k in pieces:
                for j in range(n_sub):
                    i_copy(m, k, j).wait_send()

    for m in range(micro):
        for k in range(n_ch):
            out_copy(m, k).wait()

    for m in range(micro):
        for k in range(n_ch):
            for j in range(n_sub):
                if k > 0:
                    @pl.when(even & (p > 0))
                    def _():
                        h_copy(m, k, j).wait_send()

                @pl.when(jnp.logical_not(last) if k == 0 else even)
                def _():
                    f_copy(m, k, j).wait_send()

    @pl.when(jnp.logical_not(last))
    def _():
        for m in range(micro):
            for k in range(n_ch):
                for j in range(n_sub):
                    x_copy(m, k, j).wait_send()


def shards(mesh, inputs, w_in, w_out, lengths, valid):
    micro, tok, width = inputs.shape
    hd = w_out.shape[1]
    sections = mesh.shape["pipe"]
    blocks = mesh.shape["seq"]
    streams = lengths.shape[1]
    n_ch = tok // CH
    hbm = pl.BlockSpec(memory_space=pltpu.HBM)
    return pl.pallas_call(
        functools.partial(kernel, micro, tok, width, hd, sections, blocks, streams),
        out_shape=jax.ShapeDtypeStruct((1, micro, tok, width), BF),
        in_specs=[hbm] * 5,
        out_specs=hbm,
        scratch_shapes=[
            pltpu.VMEM((micro, tok, width), BF),
            pltpu.VMEM((micro, tok, width), BF),
            pltpu.VMEM((micro, tok, width), BF),
            pltpu.VMEM((width, 4 * hd), BF),
            pltpu.VMEM((hd, width), BF),
            pltpu.VMEM((tok, hd), BF),
            pltpu.VMEM((tok, hd), BF),
            pltpu.VMEM((WINDOW + tok, hd), BF),
            pltpu.VMEM((WINDOW + tok, hd), BF),
            pltpu.VMEM((tok, hd), F32),
            pltpu.VMEM((micro, n_ch, CH, WINDOW + CH), F32),
            pltpu.SMEM(lengths.shape, jnp.int32),
            pltpu.SMEM(valid.shape, jnp.int32),
            pltpu.SemaphoreType.DMA((5,)),
            pltpu.SemaphoreType.DMA((micro, n_ch)),
        ] + [pltpu.SemaphoreType.DMA((micro, n_ch, CH // SUB))] * 6,
        compiler_params=pltpu.CompilerParams(
            collective_id=0, has_side_effects=True, vmem_limit_bytes=67043328),
    )(inputs, w_in, w_out, lengths, valid)


def solution(mesh):
    in_specs = (P(None, "seq", None), P("pipe", None, None), P("pipe", None, None), P(), P())
    out_specs = P("pipe", None, "seq", None)
    return jax.shard_map(functools.partial(shards, mesh), mesh=mesh, in_specs=in_specs,
                         out_specs=out_specs, check_vma=False)
```

```python
import functools
import math

import jax
import jax.numpy as jnp
from jax import lax
from jax.experimental import pallas as pl
from jax.experimental.pallas import tpu as pltpu
from jax.sharding import PartitionSpec as P

MESH = pl.DeviceIdType.MESH

HEAD_DIM = 128
WINDOW = 512
CH = 128
SUB = 64
HELPERS = (2, 6)
BF = jnp.bfloat16
F32 = jnp.float32

norm_eps = 1e-05
out_eps = 0.001


def half_silu(h):
    h = h.astype(BF)
    return h + h * jnp.tanh(h)


def centred(x, epsilon):
    mean = jnp.mean(x, axis=-1, keepdims=True)
    cen = x - mean
    return cen, lax.rsqrt(jnp.mean(cen * cen, axis=-1, keepdims=True) + epsilon)


def kernel(micro, tok, width, hd, sections, blocks, streams,
           inp, win, wout, lens_hbm, valid_hbm, out,
           ib, ob, xin, hx, w1, w2, qb, ub, kb, vb, acc, mask, lens, valid,
           ld_sem, ib_sem, out_sem, xs, xr, hs, hr, fs, js):
    p = lax.axis_index("pipe")
    b = lax.axis_index("seq")
    heads = hd // HEAD_DIM
    span = WINDOW + CH
    n_ch = tok // CH
    n_sub = CH // SUB
    right = lax.rem(b + 1, blocks)
    left = lax.rem(b + blocks - 1, blocks)
    up = lax.rem(p + 1, sections)
    down = lax.rem(p + sections - 1, sections)
    even = lax.rem(p, 2) == 0
    last = p == sections - 1

    barrier = pltpu.get_barrier_semaphore()
    for dev in ((p, left), (p, right), (up, b), (down, b), (up, right), (down, left)):
        pl.semaphore_signal(barrier, inc=1, device_id=dev, device_id_type=MESH)

    @pl.when(p == 0)
    def _():
        for helper in HELPERS:
            pl.semaphore_signal(barrier, inc=1, device_id=(helper, left), device_id_type=MESH)

    first_sends = {0: [(0, 3), (0, 1)], HELPERS[0]: [(0, 2), (1, 3), (1, 1)],
                   HELPERS[1]: [(0, 0), (1, 2), (1, 0)]}

    def first_load(pieces, n):
        m, k = pieces[n]
        return pltpu.make_async_copy(
            inp.at[m, k * CH:(k + 1) * CH], ib.at[n * CH:(n + 1) * CH], ib_sem.at[n])

    load_x = pltpu.make_async_copy(inp, xin, ld_sem.at[0])
    load_in = pltpu.make_async_copy(win.at[0], w1, ld_sem.at[1])
    load_out = pltpu.make_async_copy(wout.at[0], w2, ld_sem.at[2])
    load_len = pltpu.make_async_copy(lens_hbm, lens, ld_sem.at[3])
    load_val = pltpu.make_async_copy(valid_hbm, valid, ld_sem.at[4])

    @pl.when(p == 0)
    def _():
        load_x.start()

    for sender, pieces in first_sends.items():
        @pl.when(p == sender)
        def _():
            for n in range(len(pieces)):
                first_load(pieces, n).start()

    load_len.start()
    load_val.start()
    load_in.start()
    load_out.start()

    def sub_rows(k, j):
        return pl.ds(pl.multiple_of(k * CH + j * SUB, SUB), SUB)

    def x_copy(m, k, j):
        return pltpu.make_async_remote_copy(
            src_ref=ob.at[m, sub_rows(k, j)], dst_ref=xin.at[m, sub_rows(k, j)],
            send_sem=xs.at[m, k, j], recv_sem=xr.at[m, k, j],
            device_id=(up, b), device_id_type=MESH)

    def h_copy(m, k, j):
        return pltpu.make_async_remote_copy(
            src_ref=xin.at[m, sub_rows(k, j)], dst_ref=hx.at[m, sub_rows(k, j)],
            send_sem=hs.at[m, k, j], recv_sem=hr.at[m, k, j],
            device_id=(p, right), device_id_type=MESH)

    def i_copy(m, k, j, n):
        return pltpu.make_async_remote_copy(
            src_ref=ib.at[sub_rows(n, j)], dst_ref=hx.at[m, sub_rows(k, j)],
            send_sem=js.at[m, k, j], recv_sem=hr.at[m, k, j],
            device_id=(0, right), device_id_type=MESH)

    def f_copy(m, k, j):
        return pltpu.make_async_remote_copy(
            src_ref=ob.at[m, sub_rows(k, j)], dst_ref=hx.at[m, sub_rows(k, j)],
            send_sem=fs.at[m, k, j], recv_sem=hr.at[m, k, j],
            device_id=(up, right), device_id_type=MESH)

    def rows_of(k):
        return pl.ds(pl.multiple_of(k * CH, CH), CH)

    def out_copy(m, k):
        return pltpu.make_async_copy(
            ob.at[m, rows_of(k)], out.at[0, m, rows_of(k)], out_sem.at[m, k])

    for sender, pieces in first_sends.items():
        @pl.when(p == sender)
        def _():
            for n in range(len(pieces)):
                first_load(pieces, n).wait()

    helps = (p == HELPERS[0]) | (p == HELPERS[1])
    pl.semaphore_wait(barrier, jnp.where(helps, 7, 6))

    for sender, pieces in first_sends.items():
        @pl.when(p == sender)
        def _():
            for n, (m, k) in enumerate(pieces):
                for j in range(n_sub):
                    i_copy(m, k, j, n).start()

    @pl.when(p == 0)
    def _():
        load_x.wait()

    load_len.wait()
    load_val.wait()

    score_scale = 0.5 / math.sqrt(HEAD_DIM)
    ii = lax.broadcasted_iota(jnp.int32, (CH, 1), 0)
    jj = lax.broadcasted_iota(jnp.int32, (1, span), 1)

    def make_mask(step, carry):
        m = step // n_ch
        k = lax.rem(step, n_ch)
        row = k * CH + ii
        col = k * CH + jj - WINDOW
        q_pos = b * tok + row
        k_pos = b * tok + col
        q_stream = jnp.zeros_like(q_pos)
        k_stream = jnp.zeros_like(k_pos)
        bound = jnp.int32(0)
        for n in range(streams):
            bound = bound + lens[m, n]
            q_stream = q_stream + jnp.where(q_pos >= bound, 1, 0)
            k_stream = k_stream + jnp.where(k_pos >= bound, 1, 0)
        here = valid[m, b]
        before = valid[m, left]
        k_count = jnp.where(col >= 0, here, before)
        k_row = jnp.where(col >= 0, col, col + tok)
        k_code = jnp.where((k_row < k_count) & (k_pos >= 0), k_stream, -1)
        q_code = jnp.where(row < here, q_stream, -2)
        ok = (q_code == k_code) & (jj > ii) & (jj <= ii + WINDOW)
        mask[m, k] = jnp.where(ok, score_scale, 0.0)
        return carry

    lax.fori_loop(0, micro * n_ch, make_mask, 0)
    load_in.wait()
    load_out.wait()

    def project(x, targets):
        cen, rstd = centred(x.astype(F32), norm_eps)
        cen = cen.astype(BF)
        for ref, at, rows in targets:
            ref[rows] = half_silu(jnp.dot(
                cen, w1[:, at * hd:(at + 1) * hd], preferred_element_type=F32) * (0.5 * rstd))

    def weigh(m, q, lo, hi):
        rows = slice(q * CH, (q + 1) * CH)
        keys = slice(lo * CH, hi * CH)
        mk = mask[m, q, :, (lo - q) * CH:(hi - q) * CH]
        raw = [lax.dot_general(qb[rows, c], kb[keys, c], (((1,), (1,)), ((), ())),
                               preferred_element_type=F32) for c in head_cols]
        return lo, hi, [half_silu(s * mk) for s in raw]

    def mix(weighed):
        lo, hi, weights = weighed
        keys = slice(lo * CH, hi * CH)
        return jnp.concatenate([jnp.dot(w, vb[keys, c], preferred_element_type=F32)
                                for w, c in zip(weights, head_cols)], 1)

    head_cols = [slice(h * HEAD_DIM, (h + 1) * HEAD_DIM) for h in range(heads)]
    lead = WINDOW // CH

    def chunk(k):
        return slice(k * CH, (k + 1) * CH)

    def gather_weights(m, j):
        return [(q, weigh(m, q, lead + j, lead + j + 1)) for q in range(j, n_ch)]

    def gather_mix(j, weighed):
        for q, w in weighed:
            acc[chunk(q)] = mix(w) if q == j else acc[chunk(q)] + mix(w)

    def own(m, k):
        @pl.when(p > 0)
        def _():
            for j in range(n_sub):
                x_copy(m, k, j).wait_recv()

                @pl.when(even)
                def _():
                    h_copy(m, k, j).start()

        weighed = gather_weights(m, k + 1) if 0 < k < n_ch - 1 else None
        at = chunk(lead + k)
        project(xin[m, chunk(k)],
                ((kb, 3, at), (vb, 1, at), (qb, 2, chunk(k)), (ub, 0, chunk(k))))
        if weighed:
            gather_mix(k + 1, weighed)

    def halo(m, k):
        for j in range(n_sub):
            h_copy(m, k, j).wait_recv()

    def attend(m, k):
        rows = chunk(k)
        if k == n_ch - 1:
            tail = weigh(m, k, k, lead + 1)
            more = weigh(m, k - 1, k, lead + 1)
            att = acc[rows] + mix(tail)
            got = mix(more)
        else:
            halo(m, k)
            ahead = weigh(m, k - 1, k + 1, lead + 1) if k > 0 else None
            project(hx[m, rows], ((kb, 3, rows), (vb, 1, rows)))
            att = acc[rows]
            if ahead:
                got = mix(ahead)
            tail = weigh(m, k, k, k + 1)
            if ahead:
                more = weigh(m, k - 1, k, k + 1)
            att = att + mix(tail)
            if ahead:
                got = got + mix(more)
        if k > 0:
            acc[chunk(k - 1)] = got if k == 1 else acc[chunk(k - 1)] + got
        cen, rstd = centred(att, out_eps * WINDOW)
        gated = (cen * ub[rows].astype(F32)).astype(BF)
        res = xin[m, rows].astype(F32) + rstd * jnp.dot(
            gated, w2[...], preferred_element_type=F32)
        ob[m, rows] = res.astype(BF)
        out_copy(m, k).start()

        @pl.when(jnp.logical_not(last))
        def _():
            for j in range(n_sub):
                x_copy(m, k, j).start()

        @pl.when(even)
        def _():
            for j in range(n_sub):
                f_copy(m, k, j).start()

    def layer(m, carry):
        for k in range(n_ch - 1, -1, -1):
            if k == 0:
                gather_mix(1, gather_weights(m, 1))
                halo(m, n_ch - 1)
                top = chunk(n_ch - 1)
                project(hx[m, top], ((kb, 3, top), (vb, 1, top)))
            own(m, k)
        for k in range(n_ch - 1, -1, -1):
            attend(m, k)
        return carry

    lax.fori_loop(0, micro, layer, 0)

    for sender, pieces in first_sends.items():
        @pl.when(p == sender)
        def _():
            for n, (m, k) in enumerate(pieces):
                for j in range(n_sub):
                    i_copy(m, k, j, n).wait_send()

    for m in range(micro):
        for k in range(n_ch):
            out_copy(m, k).wait()

    for m in range(micro):
        for k in range(n_ch):
            for j in range(n_sub):
                @pl.when(even & (p > 0))
                def _():
                    h_copy(m, k, j).wait_send()

                @pl.when(even)
                def _():
                    f_copy(m, k, j).wait_send()

    @pl.when(jnp.logical_not(last))
    def _():
        for m in range(micro):
            for k in range(n_ch):
                for j in range(n_sub):
                    x_copy(m, k, j).wait_send()


def shards(mesh, inputs, w_in, w_out, lengths, valid):
    micro, tok, width = inputs.shape
    hd = w_out.shape[1]
    sections = mesh.shape["pipe"]
    blocks = mesh.shape["seq"]
    streams = lengths.shape[1]
    n_ch = tok // CH
    hbm = pl.BlockSpec(memory_space=pltpu.HBM)
    return pl.pallas_call(
        functools.partial(kernel, micro, tok, width, hd, sections, blocks, streams),
        out_shape=jax.ShapeDtypeStruct((1, micro, tok, width), BF),
        in_specs=[hbm] * 5,
        out_specs=hbm,
        scratch_shapes=[
            pltpu.VMEM((3 * CH, width), BF),
            pltpu.VMEM((micro, tok, width), BF),
            pltpu.VMEM((micro, tok, width), BF),
            pltpu.VMEM((micro, tok, width), BF),
            pltpu.VMEM((width, 4 * hd), BF),
            pltpu.VMEM((hd, width), BF),
            pltpu.VMEM((tok, hd), BF),
            pltpu.VMEM((tok, hd), BF),
            pltpu.VMEM((WINDOW + tok, hd), BF),
            pltpu.VMEM((WINDOW + tok, hd), BF),
            pltpu.VMEM((tok, hd), F32),
            pltpu.VMEM((micro, n_ch, CH, WINDOW + CH), F32),
            pltpu.SMEM(lengths.shape, jnp.int32),
            pltpu.SMEM(valid.shape, jnp.int32),
            pltpu.SemaphoreType.DMA((5,)),
            pltpu.SemaphoreType.DMA((3,)),
            pltpu.SemaphoreType.DMA((micro, n_ch)),
        ] + [pltpu.SemaphoreType.DMA((micro, n_ch, CH // SUB))] * 6,
        compiler_params=pltpu.CompilerParams(
            collective_id=0, has_side_effects=True, vmem_limit_bytes=67043328),
    )(inputs, w_in, w_out, lengths, valid)


def solution(mesh):
    in_specs = (P(None, "seq", None), P("pipe", None, None), P("pipe", None, None), P(), P())
    out_specs = P("pipe", None, "seq", None)
    return jax.shard_map(functools.partial(shards, mesh), mesh=mesh, in_specs=in_specs,
                         out_specs=out_specs, check_vma=False)
```

```python
import functools
import math

import jax
import jax.numpy as jnp
from jax import lax
from jax.experimental import pallas as pl
from jax.experimental.pallas import tpu as pltpu
from jax.sharding import PartitionSpec as P

MESH = pl.DeviceIdType.MESH

HEAD_DIM = 128
WINDOW = 512
CH = 128
SUB = 64
HELPERS = (2, 6)
BF = jnp.bfloat16
F32 = jnp.float32

norm_eps = 1e-05
out_eps = 0.001


def half_silu(h):
    h = h.astype(BF)
    return h + h * jnp.tanh(h)


def centred(x, epsilon):
    mean = jnp.mean(x, axis=-1, keepdims=True)
    cen = x - mean
    return cen, lax.rsqrt(jnp.mean(cen * cen, axis=-1, keepdims=True) + epsilon)


def kernel(micro, tok, width, hd, sections, blocks, streams,
           inp, win, wout, lens_hbm, valid_hbm, out,
           ib, ob, xin, hx, w1, w2, qb, ub, kb, vb, acc, mask, lens, valid,
           ld_sem, ib_sem, out_sem, xs, xr, hs, hr, fs, js):
    p = lax.axis_index("pipe")
    b = lax.axis_index("seq")
    heads = hd // HEAD_DIM
    span = WINDOW + CH
    n_ch = tok // CH
    n_sub = CH // SUB
    right = lax.rem(b + 1, blocks)
    left = lax.rem(b + blocks - 1, blocks)
    up = lax.rem(p + 1, sections)
    down = lax.rem(p + sections - 1, sections)
    even = lax.rem(p, 2) == 0
    last = p == sections - 1

    barrier = pltpu.get_barrier_semaphore()
    for dev in ((p, left), (p, right), (up, b), (down, b), (up, right), (down, left)):
        pl.semaphore_signal(barrier, inc=1, device_id=dev, device_id_type=MESH)

    @pl.when(p == 0)
    def _():
        for helper in HELPERS:
            pl.semaphore_signal(barrier, inc=1, device_id=(helper, left), device_id_type=MESH)

    first_sends = {0: [(0, 3), (0, 1)], HELPERS[0]: [(0, 2), (1, 3), (1, 1)],
                   HELPERS[1]: [(0, 0), (1, 2), (1, 0)]}

    def first_load(pieces, n):
        m, k = pieces[n]
        return pltpu.make_async_copy(
            inp.at[m, k * CH:(k + 1) * CH], ib.at[n * CH:(n + 1) * CH], ib_sem.at[n])

    load_x = pltpu.make_async_copy(inp, xin, ld_sem.at[0])
    load_in = pltpu.make_async_copy(win.at[0], w1, ld_sem.at[1])
    load_out = pltpu.make_async_copy(wout.at[0], w2, ld_sem.at[2])
    load_len = pltpu.make_async_copy(lens_hbm, lens, ld_sem.at[3])
    load_val = pltpu.make_async_copy(valid_hbm, valid, ld_sem.at[4])

    @pl.when(p == 0)
    def _():
        load_x.start()

    for sender, pieces in first_sends.items():
        @pl.when(p == sender)
        def _():
            for n in range(len(pieces)):
                first_load(pieces, n).start()

    load_len.start()
    load_val.start()
    load_in.start()
    load_out.start()

    def sub_rows(k, j):
        return pl.ds(pl.multiple_of(k * CH + j * SUB, SUB), SUB)

    def x_copy(m, k, j):
        return pltpu.make_async_remote_copy(
            src_ref=ob.at[m, sub_rows(k, j)], dst_ref=xin.at[m, sub_rows(k, j)],
            send_sem=xs.at[m, k, j], recv_sem=xr.at[m, k, j],
            device_id=(up, b), device_id_type=MESH)

    def h_copy(m, k, j):
        return pltpu.make_async_remote_copy(
            src_ref=xin.at[m, sub_rows(k, j)], dst_ref=hx.at[m, sub_rows(k, j)],
            send_sem=hs.at[m, k, j], recv_sem=hr.at[m, k, j],
            device_id=(p, right), device_id_type=MESH)

    def i_copy(m, k, j, n):
        return pltpu.make_async_remote_copy(
            src_ref=ib.at[sub_rows(n, j)], dst_ref=hx.at[m, sub_rows(k, j)],
            send_sem=js.at[m, k, j], recv_sem=hr.at[m, k, j],
            device_id=(0, right), device_id_type=MESH)

    def f_copy(m, k, j):
        return pltpu.make_async_remote_copy(
            src_ref=ob.at[m, sub_rows(k, j)], dst_ref=hx.at[m, sub_rows(k, j)],
            send_sem=fs.at[m, k, j], recv_sem=hr.at[m, k, j],
            device_id=(up, right), device_id_type=MESH)

    def rows_of(k):
        return pl.ds(pl.multiple_of(k * CH, CH), CH)

    def out_copy(m, k):
        return pltpu.make_async_copy(
            ob.at[m, rows_of(k)], out.at[0, m, rows_of(k)], out_sem.at[m, k])

    for sender, pieces in first_sends.items():
        @pl.when(p == sender)
        def _():
            for n in range(len(pieces)):
                first_load(pieces, n).wait()

    helps = (p == HELPERS[0]) | (p == HELPERS[1])
    pl.semaphore_wait(barrier, jnp.where(helps, 7, 6))

    for sender, pieces in first_sends.items():
        @pl.when(p == sender)
        def _():
            for n, (m, k) in enumerate(pieces):
                for j in range(n_sub):
                    i_copy(m, k, j, n).start()

    @pl.when(p == 0)
    def _():
        load_x.wait()

    load_len.wait()
    load_val.wait()

    score_scale = 0.5 / math.sqrt(HEAD_DIM)
    ii = lax.broadcasted_iota(jnp.int32, (CH, 1), 0)
    jj = lax.broadcasted_iota(jnp.int32, (1, span), 1)

    def make_mask(step, carry):
        m = step // n_ch
        k = lax.rem(step, n_ch)
        row = k * CH + ii
        col = k * CH + jj - WINDOW
        q_pos = b * tok + row
        k_pos = b * tok + col
        q_stream = jnp.zeros_like(q_pos)
        k_stream = jnp.zeros_like(k_pos)
        bound = jnp.int32(0)
        for n in range(streams):
            bound = bound + lens[m, n]
            q_stream = q_stream + jnp.where(q_pos >= bound, 1, 0)
            k_stream = k_stream + jnp.where(k_pos >= bound, 1, 0)
        here = valid[m, b]
        before = valid[m, left]
        k_count = jnp.where(col >= 0, here, before)
        k_row = jnp.where(col >= 0, col, col + tok)
        k_code = jnp.where((k_row < k_count) & (k_pos >= 0), k_stream, -1)
        q_code = jnp.where(row < here, q_stream, -2)
        ok = (q_code == k_code) & (jj > ii) & (jj <= ii + WINDOW)
        mask[m, k] = jnp.where(ok, score_scale, 0.0)
        return carry

    lax.fori_loop(0, jnp.where(p == 0, n_ch, micro * n_ch), make_mask, 0)
    load_in.wait()
    load_out.wait()

    def prepare(x):
        cen, rstd = centred(x.astype(F32), norm_eps)
        return cen.astype(BF), rstd

    def project(x, targets):
        project_from(prepare(x), targets)

    def project_from(prepared, targets):
        cen, rstd = prepared
        for ref, at, rows in targets:
            ref[rows] = half_silu(jnp.dot(
                cen, w1[:, at * hd:(at + 1) * hd], preferred_element_type=F32) * (0.5 * rstd))

    def weigh(m, q, lo, hi):
        rows = slice(q * CH, (q + 1) * CH)
        keys = slice(lo * CH, hi * CH)
        mk = mask[m, q, :, (lo - q) * CH:(hi - q) * CH]
        raw = [lax.dot_general(qb[rows, c], kb[keys, c], (((1,), (1,)), ((), ())),
                               preferred_element_type=F32) for c in head_cols]
        return lo, hi, [half_silu(s * mk) for s in raw]

    def mix(weighed):
        lo, hi, weights = weighed
        keys = slice(lo * CH, hi * CH)
        return jnp.concatenate([jnp.dot(w, vb[keys, c], preferred_element_type=F32)
                                for w, c in zip(weights, head_cols)], 1)

    head_cols = [slice(h * HEAD_DIM, (h + 1) * HEAD_DIM) for h in range(heads)]
    lead = WINDOW // CH

    def chunk(k):
        return slice(k * CH, (k + 1) * CH)

    def gather_weights(m, j):
        return [(q, weigh(m, q, lead + j, lead + j + 1)) for q in range(j, n_ch)]

    def gather_mix(j, weighed):
        for q, w in weighed:
            acc[chunk(q)] = mix(w) if q == j else acc[chunk(q)] + mix(w)

    def own(m, k):
        @pl.when(p > 0)
        def _():
            for j in range(n_sub):
                x_copy(m, k, j).wait_recv()

                @pl.when(even)
                def _():
                    h_copy(m, k, j).start()

        weighed = gather_weights(m, k + 1) if 0 < k < n_ch - 1 else None
        at = chunk(lead + k)
        prepared = prepare(xin[m, chunk(k)])
        project_from(prepared, ((kb, 3, at), (vb, 1, at)))
        later = (qb, 2, chunk(k)), (ub, 0, chunk(k))
        if k > 0:
            project_from(prepared, later)
        if weighed:
            gather_mix(k + 1, weighed)
        return prepared, later

    def halo(m, k):
        for j in range(n_sub):
            h_copy(m, k, j).wait_recv()

    def attend(m, k, pending):
        rows = chunk(k)
        if k == n_ch - 1:
            tail = weigh(m, k, k, lead + 1)
            more = weigh(m, k - 1, k, lead + 1)
            att = acc[rows] + mix(tail)
            got = mix(more)
            project_from(*pending)
        else:
            halo(m, k)
            ahead = weigh(m, k - 1, k + 1, lead + 1) if k > 0 else None
            project(hx[m, rows], ((kb, 3, rows), (vb, 1, rows)))
            att = acc[rows]
            if ahead:
                got = mix(ahead)
            tail = weigh(m, k, k, k + 1)
            if ahead:
                more = weigh(m, k - 1, k, k + 1)
            att = att + mix(tail)
            if ahead:
                got = got + mix(more)
        if k > 0:
            acc[chunk(k - 1)] = got if k == 1 else acc[chunk(k - 1)] + got
        cen, rstd = centred(att, out_eps * WINDOW)
        gated = (cen * ub[rows].astype(F32)).astype(BF)
        res = xin[m, rows].astype(F32) + rstd * jnp.dot(
            gated, w2[...], preferred_element_type=F32)
        ob[m, rows] = res.astype(BF)
        out_copy(m, k).start()

        @pl.when(jnp.logical_not(last))
        def _():
            for j in range(n_sub):
                x_copy(m, k, j).start()

        @pl.when(even)
        def _():
            for j in range(n_sub):
                f_copy(m, k, j).start()

    def layer(m, carry):
        @pl.when((p == 0) & (m > 0))
        def _():
            lax.fori_loop(m * n_ch, (m + 1) * n_ch, make_mask, 0)

        for k in range(n_ch - 1, -1, -1):
            if k == 0:
                gather_mix(1, gather_weights(m, 1))
                halo(m, n_ch - 1)
                top = chunk(n_ch - 1)
                project(hx[m, top], ((kb, 3, top), (vb, 1, top)))
            pending = own(m, k)
        for k in range(n_ch - 1, -1, -1):
            attend(m, k, pending)
        return carry

    lax.fori_loop(0, micro, layer, 0)

    for sender, pieces in first_sends.items():
        @pl.when(p == sender)
        def _():
            for n, (m, k) in enumerate(pieces):
                for j in range(n_sub):
                    i_copy(m, k, j, n).wait_send()

    for m in range(micro):
        for k in range(n_ch):
            out_copy(m, k).wait()

    for m in range(micro):
        for k in range(n_ch):
            for j in range(n_sub):
                @pl.when(even & (p > 0))
                def _():
                    h_copy(m, k, j).wait_send()

                @pl.when(even)
                def _():
                    f_copy(m, k, j).wait_send()

    @pl.when(jnp.logical_not(last))
    def _():
        for m in range(micro):
            for k in range(n_ch):
                for j in range(n_sub):
                    x_copy(m, k, j).wait_send()


def shards(mesh, inputs, w_in, w_out, lengths, valid):
    micro, tok, width = inputs.shape
    hd = w_out.shape[1]
    sections = mesh.shape["pipe"]
    blocks = mesh.shape["seq"]
    streams = lengths.shape[1]
    n_ch = tok // CH
    hbm = pl.BlockSpec(memory_space=pltpu.HBM)
    return pl.pallas_call(
        functools.partial(kernel, micro, tok, width, hd, sections, blocks, streams),
        out_shape=jax.ShapeDtypeStruct((1, micro, tok, width), BF),
        in_specs=[hbm] * 5,
        out_specs=hbm,
        scratch_shapes=[
            pltpu.VMEM((3 * CH, width), BF),
            pltpu.VMEM((micro, tok, width), BF),
            pltpu.VMEM((micro, tok, width), BF),
            pltpu.VMEM((micro, tok, width), BF),
            pltpu.VMEM((width, 4 * hd), BF),
            pltpu.VMEM((hd, width), BF),
            pltpu.VMEM((tok, hd), BF),
            pltpu.VMEM((tok, hd), BF),
            pltpu.VMEM((WINDOW + tok, hd), BF),
            pltpu.VMEM((WINDOW + tok, hd), BF),
            pltpu.VMEM((tok, hd), F32),
            pltpu.VMEM((micro, n_ch, CH, WINDOW + CH), F32),
            pltpu.SMEM(lengths.shape, jnp.int32),
            pltpu.SMEM(valid.shape, jnp.int32),
            pltpu.SemaphoreType.DMA((5,)),
            pltpu.SemaphoreType.DMA((3,)),
            pltpu.SemaphoreType.DMA((micro, n_ch)),
        ] + [pltpu.SemaphoreType.DMA((micro, n_ch, CH // SUB))] * 6,
        compiler_params=pltpu.CompilerParams(
            collective_id=0, has_side_effects=True, vmem_limit_bytes=67043328),
    )(inputs, w_in, w_out, lengths, valid)


def solution(mesh):
    in_specs = (P(None, "seq", None), P("pipe", None, None), P("pipe", None, None), P(), P())
    out_specs = P("pipe", None, "seq", None)
    return jax.shard_map(functools.partial(shards, mesh), mesh=mesh, in_specs=in_specs,
                         out_specs=out_specs, check_vma=False)
```
